32 devices in a mesh: seq: 8 (over y, x, core), tp: 4 (over z).
Axes of the slice: x: 2, y: 2, z: 4, core: 2. Of those that a mesh axis runs over, the one named last changes fastest.
Arguments:
- hidden_in: bfloat16 [2, 4096, 2560], P(None, 'seq'), may hold values from -6 to 6
- gate_proj: bfloat16 [2560, 5120], P(None, 'tp'), may hold values from -0.125 to 0.125
- value_proj: bfloat16 [2560, 5120], P(None, 'tp'), may hold values from -0.125 to 0.125
- bc_proj: bfloat16 [2560, 256], P(None, 'tp'), may hold values from -0.125 to 0.125
- step_proj: bfloat16 [2560, 80], P(None, 'tp'), may hold values from -0.125 to 0.125
- value_conv: float32 [4, 5120], P(None, 'tp'), may hold values from -3 to 3
- bc_conv: float32 [4, 256], replicated, may hold values from -3 to 3
- step_bias: float32 [80], P('tp'), may hold values from -1.5 to 0
- log_rate: float32 [80], P('tp'), as said below
- norm_gain: float32 [5120], P('tp'), may hold values from 0.25 to 1.75
Outputs:
- mixer_out: bfloat16 [2, 4096, 5120], P(None, 'seq', 'tp')
The draws below stay inside these ranges and needn't reach their ends.
Inputs may be any that keep to these rules, and one draw needn't show every extreme that they name: log_rate lies between -1.5 - ln(4096) and 1.0 - ln(4096).
All inputs are finite; a program needn't handle non-finite values.
Results may differ from the reference program's by a relative error of at most 0.0095.
Values may be sent and summed in bfloat16 or wider, within the bound.
A program may use at most 128 MiB of HBM per device.

```python
import math
import jax
import jax.numpy as jnp
from jax import lax

D = 2560
DI = 5120
HEADS = 80
HEAD_DIM = 64
STATE = 128
CONV = 4
BATCH = 2
BLOCK = 64
SEQ_LEN = 4096


def draw_log_rate(key, part):
    shift = math.log(SEQ_LEN)
    return jax.random.uniform(key, (HEADS,), jnp.float32, -1.5 - shift, 1.0 - shift)


def level_of(own_key, dims, cuts, smallest, top_value):
    def one(axis_at, blocks):
        draws = jax.random.uniform(jax.random.fold_in(jax.random.fold_in(own_key, 6), axis_at), (blocks,), jnp.float32, smallest / len(cuts), top_value / len(cuts))
        return jnp.repeat(jnp.exp(draws), dims[axis_at] // blocks).reshape((-1,) + (1,) * (len(dims) - axis_at - 1))

    level = one(*cuts[0])
    for cut in cuts[1:]:
        level = level * one(*cut)
    return level


def noise(rng, extent, deviation, reach, shards=(), kind=jnp.bfloat16):
    entries = deviation * jax.random.normal(rng, extent, jnp.float32)
    if shards:
        entries = entries * level_of(rng, extent, shards, -0.22, 0.18)
    return jnp.clip(entries, -reach, reach).astype(kind)


def setup_inputs(seed: int = 0) -> dict:
    streams_of = jax.random.split(jax.random.key(seed), 11)
    hidden_in = noise(streams_of[0], (BATCH, SEQ_LEN, D), 1.0, 6.0, ((1, 8),))
    gate_proj = noise(streams_of[1], (D, DI), D ** -0.5, 0.125, ((1, 4),))
    value_proj = noise(streams_of[2], (D, DI), D ** -0.5, 0.125, ((1, 4),))
    bc_proj = noise(streams_of[3], (D, 2 * STATE), D ** -0.5, 0.125, ((1, 4),))
    step_proj = noise(streams_of[4], (D, HEADS), D ** -0.5, 0.125, ((1, 4),))
    value_conv = noise(streams_of[5], (CONV, DI), CONV ** -0.5, 3.0, ((1, 4),), jnp.float32)
    bc_conv = noise(streams_of[6], (CONV, 2 * STATE), CONV ** -0.5, 3.0, (), jnp.float32)
    step_bias = jnp.clip(-1.5 + 1.5 * jax.random.uniform(streams_of[7], (HEADS,), jnp.float32) ** level_of(streams_of[7], (HEADS,), ((0, 4),), -0.2, 0.2), -1.5, 0.0)
    log_rate = draw_log_rate(jax.random.fold_in(streams_of[10], 71), 0)
    norm_gain = jnp.clip(1.0 + 0.15 * jax.random.normal(streams_of[9], (DI,), jnp.float32), 0.25, 1.75)
    return {"hidden_in": hidden_in, "gate_proj": gate_proj, "value_proj": value_proj, "bc_proj": bc_proj, "step_proj": step_proj, "value_conv": value_conv, "bc_conv": bc_conv, "step_bias": step_bias, "log_rate": log_rate, "norm_gain": norm_gain}


epsilon = 1e-05

def conv_silu(padded, kernel, length):
    running = jnp.zeros((padded.shape[0], length, padded.shape[2]), jnp.float32)
    for tap_index in range(kernel.shape[0]):
        running = running + kernel[tap_index] * padded[:, tap_index:tap_index + length, :]
    return jax.nn.silu(running)

def block_step(carried, inputs):
    values, log_decay, step_sizes, b_rows, c_rows = inputs
    length = log_decay.shape[1]
    cumulative = jnp.cumsum(log_decay, axis=1)
    log_gap = cumulative[:, :, None, :] - cumulative[:, None, :, :]
    causal = jnp.arange(length)[:, None] >= jnp.arange(length)[None, :]
    weights_in = jnp.exp(jnp.where(causal[None, :, :, None], log_gap, -jnp.inf))
    scores = jnp.einsum('bin,bjn->bij', c_rows, b_rows, precision=lax.Precision.HIGHEST)
    mixing = scores[:, :, :, None] * weights_in * step_sizes[:, None, :, :]
    within = jnp.einsum('bijh,bjhp->bihp', mixing, values, precision=lax.Precision.HIGHEST)
    earlier = jnp.einsum('bin,bhpn->bihp', c_rows, carried, precision=lax.Precision.HIGHEST)
    earlier = earlier * jnp.exp(cumulative)[..., None]
    remain = jnp.exp(cumulative[:, -1:, :] - cumulative) * step_sizes
    added_state = jnp.einsum('bjh,bjhp,bjn->bhpn', remain, values, b_rows, precision=lax.Precision.HIGHEST)
    updated = jnp.exp(cumulative[:, -1, :])[:, :, None, None] * carried + added_state
    return (updated, within + earlier)

def to_blocks(series, batch_size, blocks):
    return jnp.moveaxis(series.reshape((batch_size, blocks, BLOCK) + series.shape[2:]), 1, 0)

def reference(hidden_in, gate_proj, value_proj, bc_proj, step_proj, value_conv, bc_conv, step_bias, log_rate, norm_gain):
    flat_rows = hidden_in.reshape(-1, D)
    gate_pre = jnp.dot(flat_rows, gate_proj, preferred_element_type=jnp.float32).astype(jnp.bfloat16)
    value_pre = jnp.dot(flat_rows, value_proj, preferred_element_type=jnp.float32).astype(jnp.bfloat16)
    bc_pre = jnp.dot(flat_rows, bc_proj, preferred_element_type=jnp.float32).astype(jnp.bfloat16)
    step_pre = jnp.dot(flat_rows, step_proj, preferred_element_type=jnp.float32)
    value_pad = jnp.pad(value_pre.reshape(BATCH, SEQ_LEN, DI).astype(jnp.float32), ((0, 0), (CONV - 1, 0), (0, 0)))
    bc_pad = jnp.pad(bc_pre.reshape(BATCH, SEQ_LEN, 2 * STATE).astype(jnp.float32), ((0, 0), (CONV - 1, 0), (0, 0)))
    values = conv_silu(value_pad, value_conv, SEQ_LEN).reshape(BATCH, SEQ_LEN, HEADS, HEAD_DIM)
    bc_rows = conv_silu(bc_pad, bc_conv, SEQ_LEN)
    b_rows = bc_rows[..., :STATE]
    c_rows = bc_rows[..., STATE:]
    step_sizes = jax.nn.softplus(step_pre.reshape(BATCH, SEQ_LEN, HEADS) + step_bias)
    log_decay = -step_sizes * jnp.exp(log_rate)
    blocks = SEQ_LEN // BLOCK
    initial = jnp.zeros((BATCH, HEADS, HEAD_DIM, STATE), jnp.float32)
    final_state, outputs = lax.scan(block_step, initial, (to_blocks(values, BATCH, blocks), to_blocks(log_decay, BATCH, blocks), to_blocks(step_sizes, BATCH, blocks), to_blocks(b_rows, BATCH, blocks), to_blocks(c_rows, BATCH, blocks)))
    mixed_out = jnp.moveaxis(outputs, 0, 1).reshape(BATCH, SEQ_LEN, DI)
    gated_out = mixed_out * jax.nn.silu(gate_pre.reshape(BATCH, SEQ_LEN, DI).astype(jnp.float32))
    scale_sq = lax.optimization_barrier(jnp.sum(gated_out * gated_out, axis=-1, keepdims=True)) / DI
    return (gated_out * lax.rsqrt(scale_sq + epsilon) * norm_gain).astype(jnp.bfloat16)
```

```python
import jax
import jax.numpy as jnp
from jax import lax
from jax.experimental import pallas as pl
from jax.experimental.pallas import tpu as pltpu
from jax.sharding import PartitionSpec as P

DI = 5120
HEAD_DIM = 64
STATE = 128
CONV = 4
BLOCK = 64
PAD = 8

epsilon = 1e-05
F32 = jnp.float32
BF16 = jnp.bfloat16


def shifted(block, axis, distance):
    count = lax.axis_size(axis)
    route = [(i, i + distance) for i in range(count - distance)]
    return lax.ppermute(block, axis, route)


def silu(x):
    return x * (1.0 / (1.0 + jnp.exp(-x)))


def spread(x, expand):
    high = x.astype(BF16)
    low = (x - high.astype(F32)).astype(BF16)
    return jnp.dot(jnp.concatenate([high, low], axis=1), expand, preferred_element_type=F32)


def tile_of(width):
    return 256 if width % 256 == 0 else 128


def state_kernel(
    pre_ref, pre_halo_ref, bc_ref, bc_halo_ref, step_ref, kernel_ref, bc_kernel_ref,
    bias_ref, rate_ref, expand_ref,
    scaled_ref, bc_out_ref, fout_ref, em_ref, state_ref, decay_ref,
    window, bc_window, lows,
):
    length, width = pre_ref.shape[1], pre_ref.shape[2]
    tile = tile_of(width)
    window[0:PAD, :] = pre_halo_ref[0].astype(F32)
    bc_window[0:PAD, :] = bc_halo_ref[0].astype(F32)
    state_ref[...] = jnp.zeros_like(state_ref)
    heads = bias_ref.shape[1]
    rows = lax.broadcasted_iota(jnp.int32, (BLOCK, BLOCK), 0)
    cols = lax.broadcasted_iota(jnp.int32, (BLOCK, BLOCK), 1)
    triangle = jnp.where(rows >= cols, 1.0, 0.0).astype(F32)
    lows[...] = jnp.zeros_like(lows)

    @pl.loop(0, length // BLOCK)
    def _(index):
        at = pl.ds(pl.multiple_of(index * BLOCK, BLOCK), BLOCK)
        step_pre = step_ref[0, at, :] + bias_ref[...]
        steps = jnp.maximum(step_pre, 0.0) + jnp.log1p(jnp.exp(-jnp.abs(step_pre)))
        log_decay = -steps * jnp.exp(rate_ref[...])
        cumulative = jnp.dot(
            triangle, log_decay, precision=lax.Precision.HIGHEST, preferred_element_type=F32
        )
        last = cumulative[BLOCK - 1 : BLOCK, :]
        lows[0:1, :] += last
        mid = 0.5 * last
        fin = jnp.exp(mid - cumulative) * steps
        fout_ref[0, at, :] = jnp.exp(cumulative - mid)
        em = jnp.broadcast_to(jnp.exp(mid), (8, heads))
        em_ref[0, pl.ds(pl.multiple_of(index * 8, 8), 8), :] = em
        wide_fin = spread(fin, expand_ref[...])
        wide_em = spread(em, expand_ref[...])[0:1, :]

        bc_window[PAD:, :] = bc_ref[0, at, :].astype(F32)
        bc = bc_kernel_ref[0:1, :] * bc_window[5 : 5 + BLOCK, :]
        for k in range(1, CONV):
            bc = bc + bc_kernel_ref[k : k + 1, :] * bc_window[5 + k : 5 + k + BLOCK, :]
        bc = silu(bc).astype(BF16)
        bc_out_ref[0, at, :] = bc
        bc_window[0:PAD, :] = bc_window[BLOCK : BLOCK + PAD, :]
        b_rows = bc[:, :STATE]

        for start in range(0, width, tile):
            cut = slice(start, start + tile)
            window[PAD:, cut] = pre_ref[0, at, cut].astype(F32)
            x = kernel_ref[0:1, cut] * window[5 : 5 + BLOCK, cut]
            for k in range(1, CONV):
                x = x + kernel_ref[k : k + 1, cut] * window[5 + k : 5 + k + BLOCK, cut]
            scaled = (silu(x) * wide_fin[:, cut]).astype(BF16)
            window[0:PAD, cut] = window[BLOCK : BLOCK + PAD, cut]
            scaled_ref[0, at, cut] = scaled
            added = lax.dot_general(
                b_rows, scaled, (((0,), (0,)), ((), ())), preferred_element_type=F32
            )
            e = wide_em[:, cut]
            state_ref[0, :, cut] = e * (e * state_ref[0, :, cut] + added)

    decay_ref[0] = spread(jnp.exp(lows[...]), expand_ref[...])


def output_kernel(
    scaled_ref, bc_ref, fout_ref, em_ref, state_ref, gate_ref, expand_ref,
    gated_ref, squares_ref, held, right,
):
    length, width = scaled_ref.shape[1], scaled_ref.shape[2]
    tile = tile_of(width)
    held[...] = state_ref[0]
    rows = lax.broadcasted_iota(jnp.int32, (BLOCK, BLOCK), 0)
    cols = lax.broadcasted_iota(jnp.int32, (BLOCK, BLOCK), 1)

    @pl.loop(0, length // BLOCK)
    def _(index):
        at = pl.ds(pl.multiple_of(index * BLOCK, BLOCK), BLOCK)
        wide_fout = spread(fout_ref[0, at, :], expand_ref[...])
        em = em_ref[0, pl.ds(pl.multiple_of(index * 8, 8), 8), :]
        wide_em = spread(em, expand_ref[...])[0:1, :]
        b_rows = bc_ref[0, at, :STATE]
        c_rows = bc_ref[0, at, STATE:]
        scores = lax.dot_general(
            c_rows, b_rows, (((1,), (1,)), ((), ())), preferred_element_type=F32
        )
        mixing = jnp.where(rows >= cols, scores, 0.0).astype(BF16)
        left = jnp.concatenate([c_rows, mixing], axis=1)
        total = jnp.zeros((BLOCK, 128), F32)
        for start in range(0, width, tile):
            cut = slice(start, start + tile)
            scaled = scaled_ref[0, at, cut]
            e = wide_em[:, cut]
            entering = e * held[:, cut]
            right[:STATE, cut] = entering.astype(BF16)
            right[STATE:, cut] = scaled
            y = jnp.dot(left, right[:, cut], preferred_element_type=F32)
            added = lax.dot_general(
                b_rows, scaled, (((0,), (0,)), ((), ())), preferred_element_type=F32
            )
            held[:, cut] = e * (entering + added)
            gated = y * wide_fout[:, cut] * silu(gate_ref[0, at, cut].astype(F32))
            gated_ref[0, at, cut] = gated.astype(gated_ref.dtype)
            squared = gated * gated
            for piece in range(0, tile, 128):
                total = total + squared[:, piece : piece + 128]
        squares_ref[0, at, :] = jnp.sum(total, axis=1, keepdims=True)


def one_batch(shape):
    return pl.BlockSpec((1,) + tuple(shape[1:]), lambda b: (b,) + (0,) * (len(shape) - 1))


def whole(shape):
    return pl.BlockSpec(tuple(shape), lambda b: (0,) * len(shape))


def per_device(
    hidden_in, gate_proj, value_proj, bc_proj, step_proj,
    value_conv, bc_conv, step_bias, log_rate, norm_gain,
):
    batch, length, model_width = hidden_in.shape
    heads = step_proj.shape[1]
    width = value_proj.shape[1]
    narrow = bc_proj.shape[1]
    blocks = length // BLOCK
    flat = hidden_in.reshape(-1, model_width)
    halo_in = shifted(hidden_in[:, length - PAD :, :], "seq", 1)
    halo_flat = halo_in.reshape(-1, model_width)

    small = jnp.concatenate([bc_proj, step_proj], axis=1)
    small_pre = jnp.dot(flat, small, preferred_element_type=F32)
    step_pre = small_pre[:, narrow:].reshape(batch, length, heads)
    bc_part = small_pre[:, :narrow].astype(BF16)
    bc_halo = jnp.dot(halo_flat, bc_proj, preferred_element_type=F32).astype(BF16)
    bc_all = lax.all_gather(
        jnp.concatenate([bc_halo, bc_part], axis=0), "tp", axis=1, tiled=True
    )
    bc_halo = bc_all[: batch * PAD].reshape(batch, PAD, -1)
    bc_pre = bc_all[batch * PAD :].reshape(batch, length, -1)
    value_pre = jnp.dot(flat, value_proj, preferred_element_type=F32).astype(BF16)
    value_halo = jnp.dot(halo_flat, value_proj, preferred_element_type=F32).astype(BF16)
    value_pre = value_pre.reshape(batch, length, width)
    value_halo = value_halo.reshape(batch, PAD, width)

    lanes = lax.broadcasted_iota(jnp.int32, (2 * heads, width), 1) // HEAD_DIM
    owner = lax.broadcasted_iota(jnp.int32, (2 * heads, width), 0) % heads
    expand = (lanes == owner).astype(BF16)
    bias = step_bias.reshape(1, heads)
    rate = log_rate.reshape(1, heads)

    ins = (value_pre, value_halo, bc_pre, bc_halo, step_pre)
    fixed = (value_conv, bc_conv, bias, rate, expand)
    outs = (
        jax.ShapeDtypeStruct((batch, length, width), BF16),
        jax.ShapeDtypeStruct((batch, length, 2 * STATE), BF16),
        jax.ShapeDtypeStruct((batch, length, heads), F32),
        jax.ShapeDtypeStruct((batch, blocks * 8, heads), F32),
        jax.ShapeDtypeStruct((batch, STATE, width), F32),
        jax.ShapeDtypeStruct((batch, 8, width), F32),
    )
    scaled, bc, fout, em, local_state, decay = pl.pallas_call(
        state_kernel,
        grid=(batch,),
        out_shape=outs,
        in_specs=[one_batch(a.shape) for a in ins] + [whole(a.shape) for a in fixed],
        out_specs=[one_batch(a.shape) for a in outs],
        scratch_shapes=[
            pltpu.VMEM((BLOCK + PAD, width), F32),
            pltpu.VMEM((BLOCK + PAD, 2 * STATE), F32),
            pltpu.VMEM((8, heads), F32),
        ],
        compiler_params=pltpu.CompilerParams(vmem_limit_bytes=48 << 20),
        cost_estimate=pl.CostEstimate(
            flops=1 << 30, bytes_accessed=8 << 20, transcendentals=1 << 21
        ),
        name="state",
    )(*ins, *fixed)

    decay = decay[:, 0:1, :]
    count = lax.axis_size("seq")
    through, span = local_state, decay
    before, before_span = jnp.zeros_like(local_state), jnp.ones_like(decay)
    distance = 1
    while distance < count:
        got = shifted(through.astype(BF16), "seq", distance).astype(F32)
        before = before + before_span * got
        if 2 * distance < count:
            got_span = shifted(span, "seq", distance)
            through = through + span * got
            has = lax.axis_index("seq") >= distance
            got_span = jnp.where(has, got_span, 1.0)
            before_span = before_span * got_span
            span = span * got_span
        distance *= 2

    gate_pre = jnp.dot(flat, gate_proj, preferred_element_type=F32).astype(BF16)
    gate_pre = gate_pre.reshape(batch, length, width)
    ins = (scaled, bc, fout, em, before, gate_pre)
    outs = (
        jax.ShapeDtypeStruct((batch, length, width), BF16),
        jax.ShapeDtypeStruct((batch, length, 1), F32),
    )
    gated, squares = pl.pallas_call(
        output_kernel,
        grid=(batch,),
        out_shape=outs,
        in_specs=[one_batch(a.shape) for a in ins] + [whole(expand.shape)],
        out_specs=[one_batch(a.shape) for a in outs],
        scratch_shapes=[
            pltpu.VMEM((STATE, width), F32),
            pltpu.VMEM((STATE + BLOCK, width), BF16),
        ],
        compiler_params=pltpu.CompilerParams(vmem_limit_bytes=48 << 20),
        cost_estimate=pl.CostEstimate(
            flops=1 << 30, bytes_accessed=8 << 20, transcendentals=1 << 21
        ),
        name="outputs",
    )(*ins, expand)
    whole_sq = lax.psum(squares, "tp")
    scale = lax.rsqrt(whole_sq / DI + epsilon)
    return (gated.astype(F32) * scale * norm_gain).astype(BF16)


def solution(mesh):
    return jax.shard_map(
        per_device,
        mesh=mesh,
        in_specs=(
            P(None, "seq", None),
            P(None, "tp"),
            P(None, "tp"),
            P(None, "tp"),
            P(None, "tp"),
            P(None, "tp"),
            P(),
            P("tp"),
            P("tp"),
            P("tp"),
        ),
        out_specs=P(None, "seq", "tp"),
        check_vma=False,
    )
```

```python
import jax
import jax.numpy as jnp
from jax import lax
from jax.experimental import pallas as pl
from jax.experimental.pallas import tpu as pltpu
from jax.sharding import PartitionSpec as P

DI = 5120
HEAD_DIM = 64
STATE = 128
CONV = 4
BLOCK = 64
PAD = 16
FIRST = PAD - CONV + 1
MESH = pl.DeviceIdType.MESH

epsilon = 1e-05
F32 = jnp.float32
BF16 = jnp.bfloat16


def shifted(block, axis, distance):
    count = lax.axis_size(axis)
    route = [(i, i + distance) for i in range(count - distance)]
    return lax.ppermute(block, axis, route)


def silu(x):
    return x * (1.0 / (1.0 + jnp.exp(-x)))


def spread(x, expand):
    high = x.astype(BF16)
    low = (x - high.astype(F32)).astype(BF16)
    return jnp.dot(jnp.concatenate([high, low], axis=1), expand, preferred_element_type=F32)


def tile_of(width):
    return 256 if width % 256 == 0 else 128


def state_kernel(
    pre_ref, bc_ref, step_ref, kernel_ref, bc_kernel_ref,
    bias_ref, rate_ref, expand_ref,
    scaled_ref, bc_out_ref, fout_ref, em_ref, state_out_ref, decay_ref,
    window, bc_window, lows, state_ref,
):
    length, width = step_ref.shape[1], pre_ref.shape[2]
    tile = tile_of(width)
    window[0:PAD, :] = pre_ref[0, 0:PAD, :].astype(F32)
    bc_window[0:PAD, :] = bc_ref[0, 0:PAD, :].astype(F32)
    state_ref[...] = jnp.zeros_like(state_ref)
    heads = bias_ref.shape[1]
    rows = lax.broadcasted_iota(jnp.int32, (BLOCK, BLOCK), 0)
    cols = lax.broadcasted_iota(jnp.int32, (BLOCK, BLOCK), 1)
    triangle = jnp.where(rows >= cols, 1.0, 0.0).astype(F32)
    lows[...] = jnp.zeros_like(lows)

    @pl.loop(0, length // BLOCK)
    def _(index):
        at = pl.ds(pl.multiple_of(index * BLOCK, BLOCK), BLOCK)
        past = pl.ds(pl.multiple_of(index * BLOCK + PAD, PAD), BLOCK)
        step_pre = step_ref[0, at, :] + bias_ref[...]
        steps = jnp.maximum(step_pre, 0.0) + jnp.log1p(jnp.exp(-jnp.abs(step_pre)))
        log_decay = -steps * jnp.exp(rate_ref[...])
        cumulative = jnp.dot(
            triangle, log_decay, precision=lax.Precision.HIGHEST, preferred_element_type=F32
        )
        last = cumulative[BLOCK - 1 : BLOCK, :]
        lows[0:1, :] += last
        mid = 0.5 * last
        fin = jnp.exp(mid - cumulative) * steps
        fout_ref[0, at, :] = jnp.exp(cumulative - mid)
        em = jnp.broadcast_to(jnp.exp(mid), (8, heads))
        em_ref[0, pl.ds(pl.multiple_of(index * 8, 8), 8), :] = em
        wide_fin = spread(fin, expand_ref[...])
        wide_em = spread(em, expand_ref[...])[0:1, :]

        bc_window[PAD:, :] = bc_ref[0, past, :].astype(F32)
        bc = bc_kernel_ref[0:1, :] * bc_window[FIRST : FIRST + BLOCK, :]
        for k in range(1, CONV):
            bc = bc + bc_kernel_ref[k : k + 1, :] * bc_window[FIRST + k : FIRST + k + BLOCK, :]
        bc = silu(bc).astype(BF16)
        bc_out_ref[0, at, :] = bc
        bc_window[0:PAD, :] = bc_window[BLOCK : BLOCK + PAD, :]
        b_rows = bc[:, :STATE]

        for start in range(0, width, tile):
            cut = slice(start, start + tile)
            window[PAD:, cut] = pre_ref[0, past, cut].astype(F32)
            x = kernel_ref[0:1, cut] * window[FIRST : FIRST + BLOCK, cut]
            for k in range(1, CONV):
                x = x + kernel_ref[k : k + 1, cut] * window[FIRST + k : FIRST + k + BLOCK, cut]
            scaled = (silu(x) * wide_fin[:, cut]).astype(BF16)
            window[0:PAD, cut] = window[BLOCK : BLOCK + PAD, cut]
            scaled_ref[0, at, cut] = scaled
            added = lax.dot_general(
                b_rows, scaled, (((0,), (0,)), ((), ())), preferred_element_type=F32
            )
            e = wide_em[:, cut]
            state_ref[:, cut] = e * (e * state_ref[:, cut] + added)

    state_out_ref[0] = state_ref[...].astype(BF16)
    decay_ref[0] = spread(jnp.exp(lows[...]), expand_ref[...])


def value_kernel(
    hidden_ref, halo_ref, bc_ref, weight_ref,
    pre_ref, bc_out_ref,
    rows, slots, load_sem, send_sem, recv_sem,
):
    batch = hidden_ref.shape[0]
    count = slots.shape[0]
    narrow = bc_ref.shape[1]
    me = lax.axis_index("tp")
    step = pl.program_id(0)

    def sends():
        for away in range(1, count):
            peer = lax.rem(me + away, count)
            yield pltpu.make_async_remote_copy(
                src_ref=bc_ref, dst_ref=slots.at[me],
                send_sem=send_sem.at[away - 1], recv_sem=recv_sem.at[away - 1],
                device_id={"tp": peer}, device_id_type=MESH,
            )

    @pl.when(step == 0)
    def _():
        loads = []
        for b in range(batch):
            loads.append(pltpu.make_async_copy(
                hidden_ref.at[b], rows.at[b, pl.ds(PAD, hidden_ref.shape[1])], load_sem.at[2 * b]
            ))
            loads.append(pltpu.make_async_copy(
                halo_ref.at[b], rows.at[b, pl.ds(0, PAD)], load_sem.at[2 * b + 1]
            ))
        loads.append(pltpu.make_async_copy(bc_ref, slots.at[me], load_sem.at[2 * batch]))
        for load in loads:
            load.start()
        barrier = pltpu.get_barrier_semaphore()
        for away in range(1, count):
            pl.semaphore_signal(
                barrier, inc=1, device_id={"tp": lax.rem(me + away, count)}, device_id_type=MESH
            )
        pl.semaphore_wait(barrier, count - 1)
        for send in sends():
            send.start()
        for load in loads:
            load.wait()

    @pl.loop(0, batch)
    def _(b):
        pre_ref[b] = jnp.dot(
            rows[b], weight_ref[...], preferred_element_type=F32
        ).astype(BF16)

    @pl.when(step == pl.num_programs(0) - 1)
    def _():
        for send in sends():
            send.wait()
        bc_out_ref[...] = jnp.concatenate([slots[k] for k in range(count)], axis=1)


def gate_kernel(
    hidden_ref, weight_ref, local_ref, span_ref,
    gate_ref, before_ref,
    pair, pair_span, sent, sent_span, got, got_span, entering, entering_half, reach,
    send_sem, recv_sem,
):
    step = pl.program_id(0)
    place = lax.axis_index("seq")
    chips = lax.axis_size("seq") // 2
    core = lax.rem(place, 2)
    chip = place // 2
    partner = place + 1 - 2 * core
    half = STATE // 2
    batch = local_ref.shape[0]
    mine = pl.ds(pl.multiple_of(core * half, half), half)
    distances = []
    while 2 ** len(distances) < chips:
        distances.append(2 ** len(distances))

    def copies(source, target, slot, device):
        return pltpu.make_async_remote_copy(
            src_ref=source, dst_ref=target, send_sem=send_sem.at[slot],
            recv_sem=recv_sem.at[slot], device_id={"seq": device}, device_id_type=MESH,
        )

    def pair_copies():
        return (copies(local_ref, pair, 0, partner), copies(span_ref, pair_span, 1, partner))

    def round_copies(r):
        device = lax.rem(place + 2 * distances[r], 2 * chips)
        return (
            copies(sent.at[r], got.at[r], 2 + 2 * r, device),
            copies(sent_span.at[r], got_span.at[r], 3 + 2 * r, device),
        )

    @pl.when(step == 0)
    def _():
        barrier = pltpu.get_barrier_semaphore()
        pl.semaphore_signal(barrier, inc=1, device_id={"seq": partner}, device_id_type=MESH)
        for d in distances:
            for away in (2 * d, 2 * (chips - d)):
                pl.semaphore_signal(
                    barrier, inc=1, device_id={"seq": lax.rem(place + away, 2 * chips)},
                    device_id_type=MESH,
                )
        pl.semaphore_wait(barrier, 1 + 2 * len(distances))
        for copy in pair_copies():
            copy.start()

    def start_round(r):
        @pl.when(chip + distances[r] < chips)
        def _():
            for copy in round_copies(r):
                copy.start()

    @pl.when(step == 1)
    def _():
        for copy in pair_copies():
            copy.wait()
        sent_span[0] = span_ref[...] * pair_span[...]
        reach[...] = jnp.ones_like(reach)
        for b in range(batch):
            own = local_ref[b, mine, :].astype(F32)
            other = pair[b, mine, :].astype(F32)
            first = jnp.where(core == 0, own, other)
            second = jnp.where(core == 0, other, own)
            later = jnp.where(core == 0, pair_span[b : b + 1, :], span_ref[b : b + 1, :])
            sent[0, b] = (later * first + second).astype(BF16)
            entering_half[b] = jnp.zeros((half, own.shape[1]), BF16)
        start_round(0)

    gate_ref[...] = jnp.dot(
        hidden_ref[...], weight_ref[...], preferred_element_type=F32
    ).astype(BF16)

    @pl.when(step == pl.num_programs(0) - 1)
    def _():
        for r, d in enumerate(distances):
            @pl.when(chip + d < chips)
            def _():
                for copy in round_copies(r):
                    copy.wait_send()

            more = r + 1 < len(distances)

            @pl.when(chip >= d)
            def _():
                for copy in round_copies(r):
                    copy.wait_recv()
                for b in range(batch):
                    arrived = got[r, b].astype(F32)
                    entering_half[b] = (
                        entering_half[b].astype(F32) + reach[b : b + 1, :] * arrived
                    ).astype(BF16)
                    if more:
                        sent[r + 1, b] = (
                            sent[r, b].astype(F32) + sent_span[r, b : b + 1, :] * arrived
                        ).astype(BF16)
                reach[...] = reach[...] * got_span[r]
                if more:
                    sent_span[r + 1] = sent_span[r] * got_span[r]

            if more:
                @pl.when(chip < d)
                def _():
                    sent[r + 1] = sent[r]
                    sent_span[r + 1] = sent_span[r]

                start_round(r + 1)
        last = 2 + 2 * len(distances)
        swap = copies(entering_half, entering.at[:, mine, :], last, partner)
        swap.start()
        swap.wait()
        for b in range(batch):
            entering[b, mine, :] = entering_half[b]
        for b in range(batch):
            full = entering[b].astype(F32)
            moved = pair_span[b : b + 1, :] * full + pair[b].astype(F32)
            before_ref[b] = jnp.where(core == 0, full, moved)


def output_kernel(
    scaled_ref, bc_ref, fout_ref, em_ref, state_ref, gate_ref, expand_ref, gain_ref,
    out_ref,
    held, right, gated_all, sums, others, send_sem, recv_sem,
):
    length, width = scaled_ref.shape[1], scaled_ref.shape[2]
    blocks = length // BLOCK
    tile = tile_of(width)
    step = pl.program_id(0)
    batch = pl.num_programs(0) // 2
    rows = lax.broadcasted_iota(jnp.int32, (BLOCK, BLOCK), 0)
    cols = lax.broadcasted_iota(jnp.int32, (BLOCK, BLOCK), 1)
    lane = lax.broadcasted_iota(jnp.int32, (BLOCK, 128), 1)
    count = others.shape[0] + 1
    me = lax.axis_index("tp")

    def sends():
        for away in range(1, count):
            yield pltpu.make_async_remote_copy(
                src_ref=sums, dst_ref=others.at[away - 1],
                send_sem=send_sem.at[away - 1], recv_sem=recv_sem.at[away - 1],
                device_id={"tp": lax.rem(me + away, count)}, device_id_type=MESH,
            )

    @pl.when(step == 0)
    def _():
        sums[...] = jnp.zeros_like(sums)
        barrier = pltpu.get_barrier_semaphore()
        for away in range(1, count):
            pl.semaphore_signal(
                barrier, inc=1, device_id={"tp": lax.rem(me + away, count)}, device_id_type=MESH
            )
        pl.semaphore_wait(barrier, count - 1)

    @pl.when(step < batch)
    def _():
        held[...] = state_ref[0]

        @pl.loop(0, blocks)
        def _(index):
            at = pl.ds(pl.multiple_of(index * BLOCK, BLOCK), BLOCK)
            wide_fout = spread(fout_ref[0, at, :], expand_ref[...])
            em = em_ref[0, pl.ds(pl.multiple_of(index * 8, 8), 8), :]
            wide_em = spread(em, expand_ref[...])[0:1, :]
            b_rows = bc_ref[0, at, :STATE]
            c_rows = bc_ref[0, at, STATE:]
            scores = lax.dot_general(
                c_rows, b_rows, (((1,), (1,)), ((), ())), preferred_element_type=F32
            )
            mixing = jnp.where(rows >= cols, scores, 0.0).astype(BF16)
            left = jnp.concatenate([c_rows, mixing], axis=1)
            total = jnp.zeros((BLOCK, 128), F32)
            for start in range(0, width, tile):
                cut = slice(start, start + tile)
                scaled = scaled_ref[0, at, cut]
                e = wide_em[:, cut]
                entering = e * held[:, cut]
                right[:STATE, cut] = entering.astype(BF16)
                right[STATE:, cut] = scaled
                y = jnp.dot(left, right[:, cut], preferred_element_type=F32)
                added = lax.dot_general(
                    b_rows, scaled, (((0,), (0,)), ((), ())), preferred_element_type=F32
                )
                held[:, cut] = e * (entering + added)
                gated = y * wide_fout[:, cut] * silu(gate_ref[0, at, cut].astype(F32))
                gated_all[step, at, cut] = gated
                squared = gated * gated
                for piece in range(0, tile, 128):
                    total = total + squared[:, piece : piece + 128]
            column = jnp.sum(total, axis=1, keepdims=True)
            sums[...] += jnp.where(lane == step * blocks + index, column, 0.0)

    @pl.when(step == batch - 1)
    def _():
        for send in sends():
            send.start()

    @pl.when(step == batch)
    def _():
        for send in sends():
            send.wait()

    @pl.when(step >= batch)
    def _():
        whole_sq = sums[...]
        for away in range(1, count):
            whole_sq = whole_sq + others[away - 1]
        scale = lax.rsqrt(whole_sq / DI + epsilon)

        @pl.loop(0, blocks)
        def _(index):
            at = pl.ds(pl.multiple_of(index * BLOCK, BLOCK), BLOCK)
            here = (step - batch) * blocks + index
            column = jnp.sum(jnp.where(lane == here, scale, 0.0), axis=1, keepdims=True)
            for start in range(0, width, tile):
                cut = slice(start, start + tile)
                out_ref[0, at, cut] = (
                    gated_all[step - batch, at, cut] * column * gain_ref[:, cut]
                ).astype(BF16)


def one_batch(shape):
    return pl.BlockSpec((1,) + tuple(shape[1:]), lambda b: (b,) + (0,) * (len(shape) - 1))


def whole(shape):
    return pl.BlockSpec(tuple(shape), lambda b: (0,) * len(shape))


def per_device(
    hidden_in, gate_proj, value_proj, bc_proj, step_proj,
    value_conv, bc_conv, step_bias, log_rate, norm_gain,
):
    batch, length, model_width = hidden_in.shape
    heads = step_proj.shape[1]
    width = value_proj.shape[1]
    narrow = bc_proj.shape[1]
    blocks = length // BLOCK
    tp = lax.axis_size("tp")
    tile = tile_of(width)
    flat = hidden_in.reshape(-1, model_width)
    halo_in = shifted(hidden_in[:, length - PAD :, :], "seq", 1)

    small = jnp.concatenate([bc_proj, step_proj], axis=1)
    small_pre = jnp.dot(flat, small, preferred_element_type=F32)
    step_pre = small_pre[:, narrow:].reshape(batch, length, heads)
    bc_part = small_pre[:, :narrow].astype(BF16).reshape(batch, length, narrow)
    bc_halo = jnp.dot(
        halo_in.reshape(-1, model_width), bc_proj, preferred_element_type=F32
    ).astype(BF16).reshape(batch, PAD, narrow)
    bc_part = jnp.concatenate([bc_halo, bc_part], axis=1).reshape(-1, narrow)
    hbm = pl.BlockSpec(memory_space=pl.ANY)
    padded = PAD + length
    value_pre, bc_pre = pl.pallas_call(
        value_kernel,
        grid=(width // tile,),
        out_shape=(
            jax.ShapeDtypeStruct((batch, padded, width), BF16),
            jax.ShapeDtypeStruct((batch * padded, narrow * tp), BF16),
        ),
        in_specs=[hbm, hbm, hbm, pl.BlockSpec((model_width, tile), lambda j: (0, j))],
        out_specs=[
            pl.BlockSpec((batch, padded, tile), lambda j: (0, 0, j)),
            pl.BlockSpec((batch * padded, narrow * tp), lambda j: (0, 0)),
        ],
        scratch_shapes=[
            pltpu.VMEM((batch, padded, model_width), BF16),
            pltpu.VMEM((tp, batch * padded, narrow), BF16),
            pltpu.SemaphoreType.DMA((2 * batch + 1,)),
            pltpu.SemaphoreType.DMA((tp - 1,)),
            pltpu.SemaphoreType.DMA((tp - 1,)),
        ],
        compiler_params=pltpu.CompilerParams(
            vmem_limit_bytes=48 << 20, collective_id=0, has_side_effects=True
        ),
        name="value",
    )(hidden_in, halo_in, bc_part, value_proj)
    bc_pre = bc_pre.reshape(batch, padded, narrow * tp)

    lanes = lax.broadcasted_iota(jnp.int32, (2 * heads, width), 1) // HEAD_DIM
    owner = lax.broadcasted_iota(jnp.int32, (2 * heads, width), 0) % heads
    expand = (lanes == owner).astype(BF16)
    bias = step_bias.reshape(1, heads)
    rate = log_rate.reshape(1, heads)

    ins = (value_pre, bc_pre, step_pre)
    fixed = (value_conv, bc_conv, bias, rate, expand)
    outs = (
        jax.ShapeDtypeStruct((batch, length, width), BF16),
        jax.ShapeDtypeStruct((batch, length, 2 * STATE), BF16),
        jax.ShapeDtypeStruct((batch, length, heads), F32),
        jax.ShapeDtypeStruct((batch, blocks * 8, heads), F32),
        jax.ShapeDtypeStruct((batch, STATE, width), BF16),
        jax.ShapeDtypeStruct((batch, 8, width), F32),
    )
    scaled, bc, fout, em, local_state, decay = pl.pallas_call(
        state_kernel,
        grid=(batch,),
        out_shape=outs,
        in_specs=[one_batch(a.shape) for a in ins] + [whole(a.shape) for a in fixed],
        out_specs=[one_batch(a.shape) for a in outs],
        scratch_shapes=[
            pltpu.VMEM((BLOCK + PAD, width), F32),
            pltpu.VMEM((BLOCK + PAD, 2 * STATE), F32),
            pltpu.VMEM((8, heads), F32),
            pltpu.VMEM((STATE, width), F32),
        ],
        compiler_params=pltpu.CompilerParams(vmem_limit_bytes=48 << 20),
        cost_estimate=pl.CostEstimate(
            flops=1 << 30, bytes_accessed=8 << 20, transcendentals=1 << 21
        ),
        name="state",
    )(*ins, *fixed)

    span = jnp.concatenate([decay[:, 0, :], decay[: 8 - batch, 1, :]], axis=0)
    span = jnp.pad(span, ((0, 8 - span.shape[0]), (0, 0)))
    chips = lax.axis_size("seq") // 2
    rounds = max(1, (chips - 1).bit_length())
    half = STATE // 2
    moves = 3 + 2 * rounds
    once = pl.Buffered(1)
    gate_pre, before = pl.pallas_call(
        gate_kernel,
        grid=(width // tile,),
        out_shape=(
            jax.ShapeDtypeStruct((batch * length, width), BF16),
            jax.ShapeDtypeStruct((batch, STATE, width), F32),
        ),
        in_specs=[
            pl.BlockSpec(flat.shape, lambda j: (0, 0), pipeline_mode=once),
            pl.BlockSpec((model_width, tile), lambda j: (0, j)),
            pl.BlockSpec(local_state.shape, lambda j: (0, 0, 0), pipeline_mode=once),
            pl.BlockSpec(span.shape, lambda j: (0, 0), pipeline_mode=once),
        ],
        out_specs=[
            pl.BlockSpec((batch * length, tile), lambda j: (0, j)),
            pl.BlockSpec((batch, STATE, width), lambda j: (0, 0, 0)),
        ],
        scratch_shapes=[
            pltpu.VMEM((batch, STATE, width), BF16),
            pltpu.VMEM((8, width), F32),
            pltpu.VMEM((rounds, batch, half, width), BF16),
            pltpu.VMEM((rounds, 8, width), F32),
            pltpu.VMEM((rounds, batch, half, width), BF16),
            pltpu.VMEM((rounds, 8, width), F32),
            pltpu.VMEM((batch, STATE, width), BF16),
            pltpu.VMEM((batch, half, width), BF16),
            pltpu.VMEM((8, width), F32),
            pltpu.SemaphoreType.DMA((moves,)),
            pltpu.SemaphoreType.DMA((moves,)),
        ],
        compiler_params=pltpu.CompilerParams(
            vmem_limit_bytes=56 << 20, collective_id=1, has_side_effects=True
        ),
        name="gate",
    )(flat, gate_proj, local_state, span)
    gate_pre = gate_pre.reshape(batch, length, width)

    ins = (scaled, bc, fout, em, before, gate_pre)

    def clamped(shape):
        return pl.BlockSpec(
            (1,) + tuple(shape[1:]), lambda s: (jnp.minimum(s, batch - 1), 0, 0)
        )

    gain = norm_gain.reshape(1, width)
    return pl.pallas_call(
        output_kernel,
        grid=(2 * batch,),
        out_shape=jax.ShapeDtypeStruct((batch, length, width), BF16),
        in_specs=[clamped(a.shape) for a in ins] + [whole(expand.shape), whole(gain.shape)],
        out_specs=pl.BlockSpec(
            (1, length, width), lambda s: (jnp.maximum(s - batch, 0), 0, 0)
        ),
        scratch_shapes=[
            pltpu.VMEM((STATE, width), F32),
            pltpu.VMEM((STATE + BLOCK, width), BF16),
            pltpu.VMEM((batch, length, width), F32),
            pltpu.VMEM((BLOCK, 128), F32),
            pltpu.VMEM((tp - 1, BLOCK, 128), F32),
            pltpu.SemaphoreType.DMA((tp - 1,)),
            pltpu.SemaphoreType.DMA((tp - 1,)),
        ],
        compiler_params=pltpu.CompilerParams(
            vmem_limit_bytes=56 << 20, collective_id=2, has_side_effects=True
        ),
        name="outputs",
    )(*ins, expand, gain)


def solution(mesh):
    return jax.shard_map(
        per_device,
        mesh=mesh,
        in_specs=(
            P(None, "seq", None),
            P(None, "tp"),
            P(None, "tp"),
            P(None, "tp"),
            P(None, "tp"),
            P(None, "tp"),
            P(),
            P("tp"),
            P("tp"),
            P("tp"),
        ),
        out_specs=P(None, "seq", "tp"),
        check_vma=False,
    )
```
